32 devices in a mesh: row: 2 (over y), phi: 16 (over z, x, core).
Axes of the slice: x: 2, y: 2, z: 4, core: 2. Of those that a mesh axis runs over, the one named last changes fastest.
Arguments:
- density: float32 [32, 2048, 512], P('row', 'phi'), may hold values from 0.3 to 3
- velocity: float32 [3, 32, 2048, 512], P(None, 'row', 'phi'), may hold values from -3 to 3
- magnetic: float32 [3, 32, 2048, 512], P(None, 'row', 'phi'), may hold values from -6 to 6
Outputs:
- density_next: float32 [32, 2048, 512], P('row', 'phi')
- magnetic_next: float32 [3, 32, 2048, 512], P(None, 'row', 'phi')
The draws below stay inside these ranges and needn't reach their ends.
All inputs are finite; a program needn't handle non-finite values.
Results may differ from the reference program's by a relative error of at most 0.0003.
Values sent between devices are 32-bit elements; how exact they have to be, the bound alone decides.
A program may use at most 256 MiB of HBM per device.

```python
import math
from functools import partial
import jax
import jax.numpy as jnp
from jax import lax

NP = 2048
NT = 512
NPOL = 128
NR = 32


def block_levels(key, dims, shards, low, largest):
    factor_of = 1.0
    for dim, parts in shards:
        draws = jax.random.uniform(jax.random.fold_in(jax.random.fold_in(key, 6), dim), (parts,), jnp.float32, low / len(shards), largest / len(shards))
        factor_of = factor_of * jnp.repeat(jnp.exp(draws), dims[dim] // parts).reshape((-1,) + (1,) * (len(dims) - 1 - dim))
    return factor_of


def centred(own_key, extent, scale, most, split=(), dtype=jnp.bfloat16):
    result = jax.random.normal(own_key, extent, jnp.float32) * scale
    if len(split) > 0:
        result = block_levels(own_key, extent, split, -0.22, 0.18) * result
    return jnp.clip(result, min=-most, max=most).astype(dtype)


def setup_inputs(seed: int = 0) -> dict:
    arg_keys = jax.random.split(jax.random.key(seed), 4)
    return {
        "density": jnp.clip(jnp.exp(math.log(3.0) - 2.3025851 * jax.random.uniform(arg_keys[0], (NR, NP, NT), jnp.float32) ** block_levels(arg_keys[0], (NR, NP, NT), ((0, 2), (1, 16)), -0.2, 0.2)), 0.3, 3.0),
        "velocity": centred(arg_keys[1], (3, NR, NP, NT), 0.5, 3.0, ((1, 2), (2, 16)), jnp.float32),
        "magnetic": centred(arg_keys[2], (3, NR, NP, NT), 1.0, 6.0, ((1, 2), (2, 16)), jnp.float32),
    }


COURANT_RAD = 0.3
COURANT_POL = 0.25
COURANT_AZI = 0.35
SOUND_SPEED = 1.0


def shift_theta(values, offset):
    if offset == 0:
        return values
    if offset > 0:
        border = jnp.repeat(values[..., -1:], offset, axis=-1)
        return jnp.concatenate([values[..., offset:], border], axis=-1)
    border = jnp.repeat(values[..., :1], -offset, axis=-1)
    return jnp.concatenate([border, values[..., :offset]], axis=-1)


def interface_value(outer_left, inner_left, inner_right, outer_right):
    guess = (7.0 / 12.0) * (inner_left + inner_right) - (1.0 / 12.0) * (outer_left + outer_right)
    return jnp.clip(guess, jnp.minimum(inner_left, inner_right), jnp.maximum(inner_left, inner_right))


def edge_values(nearby):
    centre = nearby(0)
    left_face = interface_value(nearby(-2), nearby(-1), centre, nearby(1))
    right_face = interface_value(nearby(-1), centre, nearby(1), nearby(2))
    to_left = left_face - centre
    to_right = right_face - centre
    left_limited = jnp.clip(to_left, -2.0 * jnp.abs(to_right), 2.0 * jnp.abs(to_right))
    right_limited = jnp.clip(to_right, -2.0 * jnp.abs(to_left), 2.0 * jnp.abs(to_left))
    return centre + left_limited, centre + right_limited


def hll_flux(dens_left, dens_right, speed_left, speed_right):
    slowest = jnp.minimum(jnp.minimum(speed_left, speed_right) - SOUND_SPEED, 0.0)
    fastest = jnp.maximum(jnp.maximum(speed_left, speed_right) + SOUND_SPEED, 0.0)
    upwind = fastest * dens_left * speed_left - slowest * dens_right * speed_right
    return (upwind + slowest * fastest * (dens_right - dens_left)) / (fastest - slowest)


def axis_divergence(dens, speed, axis, count, ghost):
    def picker(field):
        def nearby(offset):
            return lax.slice_in_dim(field, ghost - 1 + offset, ghost + 1 + offset + count, axis=axis)
        return nearby

    def window(values, start, stop):
        return lax.slice_in_dim(values, start, stop, axis=axis)

    dens_left, dens_right = edge_values(picker(dens))
    speed_left, speed_right = edge_values(picker(speed))
    flux = hll_flux(window(dens_right, 0, count + 1), window(dens_left, 1, count + 2),
                    window(speed_right, 0, count + 1), window(speed_left, 1, count + 2))
    return window(flux, 1, count + 1) - window(flux, 0, count)


def theta_divergence(dens, speed):
    dens_left, dens_right = edge_values(partial(shift_theta, dens))
    speed_left, speed_right = edge_values(partial(shift_theta, speed))
    flux = hll_flux(shift_theta(dens_right, -1), dens_left, shift_theta(speed_right, -1), speed_left)
    position = lax.broadcasted_iota(jnp.int32, flux.shape, flux.ndim - 1)
    flux = jnp.where(position == 0, jnp.zeros_like(flux), flux)
    upper_flux = jnp.concatenate([flux[..., 1:], jnp.zeros_like(flux[..., :1])], axis=-1)
    return upper_flux - flux


def advance(primitive, magnetic, ghost, face_ghost, radial, azimuth):
    dens = primitive[0]
    radial_speed = primitive[1]
    polar_speed = primitive[2]
    azimuth_speed = primitive[3]

    def inner(values, width):
        return values[width:width + radial, width:width + azimuth]

    def box(values, width):
        return values[width - 1:width + radial + 1, width - 1:width + azimuth + 1]

    rad_term = axis_divergence(dens[:, ghost:ghost + azimuth], radial_speed[:, ghost:ghost + azimuth], 0, radial, ghost)
    azi_term = axis_divergence(dens[ghost:ghost + radial], azimuth_speed[ghost:ghost + radial], 1, azimuth, ghost)
    dens_inner = inner(dens, ghost)
    pol_term = theta_divergence(dens_inner, inner(polar_speed, ghost))
    density_next = dens_inner - COURANT_RAD * rad_term - COURANT_POL * pol_term - COURANT_AZI * azi_term

    radial_span = magnetic[0][face_ghost - 1:face_ghost + radial + 2, face_ghost - 1:face_ghost + azimuth + 1]
    radial_cell = 0.5 * (radial_span[:-1] + radial_span[1:])
    azimuth_span = magnetic[2][face_ghost - 1:face_ghost + radial + 1, face_ghost - 1:face_ghost + azimuth + 2]
    azimuth_cell = 0.5 * (azimuth_span[:, :-1] + azimuth_span[:, 1:])
    polar_box = box(magnetic[1], face_ghost)
    polar_cell = 0.5 * (polar_box + shift_theta(polar_box, 1))
    speed_r = box(radial_speed, ghost)
    speed_t = box(polar_speed, ghost)
    speed_p = box(azimuth_speed, ghost)
    radial_emf = -(speed_t * azimuth_cell - speed_p * polar_cell)
    polar_emf = -(speed_p * radial_cell - speed_r * azimuth_cell)
    azimuth_emf = -(speed_r * polar_cell - speed_t * radial_cell)

    radial_edge = 0.5 * (radial_emf[1:radial + 1, :-1] + radial_emf[1:radial + 1, 1:])
    radial_below = 0.5 * (shift_theta(radial_edge, -1) + radial_edge)
    radial_above = 0.5 * (radial_edge + shift_theta(radial_edge, 1))
    azimuth_edge = 0.5 * (azimuth_emf[:-1, 1:azimuth + 1] + azimuth_emf[1:, 1:azimuth + 1])
    azimuth_below = 0.5 * (shift_theta(azimuth_edge, -1) + azimuth_edge)
    azimuth_above = 0.5 * (azimuth_edge + shift_theta(azimuth_edge, 1))
    polar_edge = 0.25 * (polar_emf[:-1, :-1] + polar_emf[1:, :-1] + polar_emf[:-1, 1:] + polar_emf[1:, 1:])

    radial_next = inner(magnetic[0], face_ghost) - COURANT_POL * (azimuth_above[:radial] - azimuth_below[:radial]) \
        + COURANT_AZI * (polar_edge[:radial, 1:] - polar_edge[:radial, :-1])
    polar_next = inner(magnetic[1], face_ghost) - COURANT_AZI * (radial_below[:, 1:] - radial_below[:, :-1]) \
        + COURANT_RAD * (azimuth_below[1:] - azimuth_below[:-1])
    azimuth_next = inner(magnetic[2], face_ghost) - COURANT_RAD * (polar_edge[1:, :azimuth] - polar_edge[:-1, :azimuth]) \
        + COURANT_POL * (radial_above[:, :azimuth] - radial_below[:, :azimuth])
    return density_next, jnp.stack([radial_next, polar_next, azimuth_next])


def pad_reference(values, width):
    values = jnp.pad(values, ((0, 0), (width, width), (0, 0), (0, 0)), mode="edge")
    return jnp.pad(values, ((0, 0), (0, 0), (width, width), (0, 0)), mode="wrap")


def reference(density, velocity, magnetic):
    half_polar = NPOL // 2
    primitive = jnp.concatenate([density[None], velocity], axis=0)
    polar_rows = jnp.concatenate([primitive[..., :half_polar], primitive[..., NT - half_polar:]], axis=-1)
    theta_row = jnp.concatenate([jnp.arange(half_polar), jnp.arange(NT - half_polar, NT)]).astype(jnp.float32)
    row_sine = jnp.sin(jnp.pi * (theta_row + 0.5) / NT)
    edge_sine = jnp.sin(jnp.pi * (half_polar + 0.5) / NT)
    mode_sine = jnp.sin(jnp.pi * jnp.arange(NP // 2 + 1).astype(jnp.float32) / NP)
    row_square = (row_sine * row_sine)[None, :]
    mode_square = (edge_sine * mode_sine)[:, None]
    damping = row_square / jnp.maximum(row_square, mode_square * mode_square)
    spectrum = jnp.fft.rfft(polar_rows, axis=2)
    smoothed = jnp.fft.irfft(spectrum * damping[None, None], n=NP, axis=2).astype(jnp.float32)
    primitive = jnp.concatenate([smoothed[..., :half_polar], primitive[..., half_polar:NT - half_polar],
                                 smoothed[..., half_polar:]], axis=-1)
    state = pad_reference(jnp.concatenate([primitive, magnetic], axis=0), 3)
    return advance(state[:4], state[4:], 3, 3, NR, NP)
```

```python
import math

import jax
import jax.numpy as jnp
import numpy as np
from jax import lax
from jax.experimental import pallas as pl
from jax.experimental.pallas import tpu as pltpu
from jax.sharding import PartitionSpec as P

NPOL = 128
RADIX = 16
FRONT = 16
TILE = 8

COURANT_RAD = 0.3
COURANT_POL = 0.25
COURANT_AZI = 0.35
SOUND_SPEED = 1.0


def rotate(value, angle):
    re, im = value
    c, s = math.cos(angle), math.sin(angle)
    if im is None:
        return (re * c, re * s)
    return (re * c - im * s, re * s + im * c)


def add(a, b, sign=1.0):
    def part(x, y):
        if y is None:
            return x
        if x is None:
            return y if sign > 0 else -y
        return x + y if sign > 0 else x - y

    return (part(a[0], b[0]), part(a[1], b[1]))


def conj(a):
    return (a[0], None if a[1] is None else -a[1])


def real_fft(xs):
    n = len(xs)
    if n == 1:
        return [(xs[0], None)]
    if n == 2:
        return [(xs[0] + xs[1], None), (xs[0] - xs[1], None)]
    even, odd = real_fft(xs[0::2]), real_fft(xs[1::2])
    half = n // 2

    def at(spec, k):
        return spec[k] if k <= half // 2 else conj(spec[half - k])

    result = []
    for k in range(half + 1):
        e, o = at(even, k % half), at(odd, k % half)
        if k == 0:
            result.append(add(e, o))
        elif k == half:
            result.append(add(e, o, -1.0))
        elif 4 * k == n:
            result.append((e[0], -o[0]))
        else:
            result.append(add(e, rotate(o, -2.0 * math.pi * k / n)))
    return result


def real_ifft(spec, n):
    if n == 2:
        a, b = spec[0][0], spec[1][0]
        return [a + b, a - b]
    half = n // 2
    even, odd = [], []
    for k in range(half // 2 + 1):
        a, b = spec[k], conj(spec[half - k])
        if k == 0:
            a, b = (spec[0][0], None), (spec[half][0], None)
            even.append(add(a, b))
            odd.append(add(a, b, -1.0))
        elif 4 * k == n:
            even.append((2.0 * spec[k][0], None))
            odd.append((-2.0 * spec[k][1], None))
        else:
            even.append(add(a, b))
            odd.append(rotate(add(a, b, -1.0), 2.0 * math.pi * k / n))
    evens, odds = real_ifft(even, half), real_ifft(odd, half)
    return [v for pair in zip(evens, odds) for v in pair]


def filter_tables(cells, theta_count):
    inner = cells // RADIX
    half_polar = NPOL // 2
    k2 = np.arange(RADIX // 2 + 1)[:, None]
    mode = k2 + RADIX * np.arange(inner)[None, :]
    angle = 2.0 * np.pi / cells * ((mode[:, :, None] * np.arange(inner)) % cells)
    cos, sin = np.cos(angle), np.sin(angle)
    forward = np.concatenate(
        [np.concatenate([cos, sin], 2), np.concatenate([-sin, cos], 2)], 1
    ).astype(np.float32)
    rows = np.arange(NPOL)
    theta = np.where(rows < half_polar, rows, theta_count - NPOL + rows)
    row_square = np.sin(np.pi * (theta + 0.5) / theta_count) ** 2
    edge = np.sin(np.pi * (half_polar + 0.5) / theta_count)
    mode_square = (edge * np.sin(np.pi * mode / cells)) ** 2
    damping = row_square / np.maximum(row_square, mode_square[:, :, None])
    return forward, (damping / cells).astype(np.float32)


def filter_kernel(group, inner, blocks, x_ref, basis_ref, damp_ref, out_ref):
    azimuth = x_ref.shape[2]

    def slab(d):
        parts = [
            x_ref[d * blocks : (d + 1) * blocks, g].reshape(inner, NPOL) for g in range(group)
        ]
        return jnp.concatenate(parts, axis=1) if group > 1 else parts[0]

    spectrum = real_fft([slab(d) for d in range(RADIX)])
    filtered = []
    for k, (re, im) in enumerate(spectrum):
        basis = basis_ref[k]
        if im is None:
            forward = basis[:, :inner]
            stacked = re
        else:
            forward = basis
            stacked = jnp.concatenate([re, im], axis=0)
        modes = jnp.dot(
            forward, stacked, precision=lax.Precision.HIGHEST, preferred_element_type=jnp.float32
        )
        damp = damp_ref[k]
        damp = jnp.concatenate([damp, damp], axis=0)
        if group > 1:
            damp = jnp.concatenate([damp] * group, axis=1)
        back = lax.dot_general(
            forward,
            modes * damp,
            (((0,), (0,)), ((), ())),
            precision=lax.Precision.HIGHEST,
            preferred_element_type=jnp.float32,
        )
        filtered.append((back, None) if im is None else (back[:inner], back[inner:]))
    for d, value in enumerate(real_ifft(filtered, RADIX)):
        for g in range(group):
            out_ref[d * blocks : (d + 1) * blocks, g] = value[
                :, g * NPOL : (g + 1) * NPOL
            ].reshape(blocks, azimuth, NPOL)


def filter_lines(lines, theta_count):
    devices, pairs, azimuth, _ = lines.shape
    cells = devices * azimuth
    inner = cells // RADIX
    blocks = inner // azimuth
    group = 2 if pairs % 2 == 0 else 1
    forward, damping = filter_tables(cells, theta_count)
    spec = pl.BlockSpec((devices, group, azimuth, NPOL), lambda p: (0, p, 0, 0))
    return pl.pallas_call(
        lambda *refs: filter_kernel(group, inner, blocks, *refs),
        grid=(pairs // group,),
        in_specs=[
            spec,
            pl.BlockSpec(forward.shape, lambda p: (0, 0, 0)),
            pl.BlockSpec(damping.shape, lambda p: (0, 0, 0)),
        ],
        out_specs=spec,
        out_shape=jax.ShapeDtypeStruct(lines.shape, jnp.float32),
        compiler_params=pltpu.CompilerParams(vmem_limit_bytes=56 * 1024 * 1024),
        name="polar_filter",
    )(lines, jnp.asarray(forward), jnp.asarray(damping))


def interface_value(outer_left, inner_left, inner_right, outer_right):
    guess = 7.0 / 12.0 * (inner_left + inner_right) - 1.0 / 12.0 * (outer_left + outer_right)
    low = jnp.minimum(inner_left, inner_right)
    return jnp.minimum(jnp.maximum(guess, low), jnp.maximum(inner_left, inner_right))


def limited(centre, left_face, right_face):
    to_left = left_face - centre
    to_right = right_face - centre
    reach_right = 2.0 * jnp.abs(to_right)
    reach_left = 2.0 * jnp.abs(to_left)
    left = jnp.minimum(jnp.maximum(to_left, -reach_right), reach_right)
    right = jnp.minimum(jnp.maximum(to_right, -reach_left), reach_left)
    return centre + left, centre + right


def edges(q):
    left_face = interface_value(q[0], q[1], q[2], q[3])
    right_face = interface_value(q[1], q[2], q[3], q[4])
    return limited(q[2], left_face, right_face)


def hll_flux(dens_left, dens_right, speed_left, speed_right):
    slowest = jnp.minimum(jnp.minimum(speed_left, speed_right) - SOUND_SPEED, 0.0)
    fastest = jnp.maximum(jnp.maximum(speed_left, speed_right) + SOUND_SPEED, 0.0)
    upwind = fastest * dens_left * speed_left - slowest * dens_right * speed_right
    return (upwind + slowest * fastest * (dens_right - dens_left)) / (fastest - slowest)


PRIM_ROWS = ((0, 0, 3), (3, 3, 3), (1, 6, 1), (2, 7, 1))
MAG_ROWS_LOW = ((4, 8, 1), (5, 9, 1), (6, 10, 1))
MAG_ROWS_HIGH = ((4, 8, 1), (5, 9, 1), (6, 10, 2))
PACKED = 16


def stencil_kernel(
    radial, azimuth, dens, vel, mag, polar, g2, g2p, g5, g5p, gbr, side, sidep,
    dens_out, mag_out,
    s0, s1, s2, s3, s4, s5, s6, er, et, ep, carry_rho, carry_u, carry_flux,
):
    state = (s0, s1, s2, s3, s4, s5, s6)
    t = pl.program_id(0)
    layer = t - 3
    width = dens.shape[-1]
    half = NPOL // 2
    slot = lax.rem(t, 8)
    own = slice(FRONT, FRONT + azimuth)

    def merge(raw, pol):
        lane = lax.broadcasted_iota(jnp.int32, pol.shape, 1)
        return jnp.concatenate(
            [
                jnp.where(lane < half, pol, raw[:, :NPOL]),
                raw[:, NPOL : width - NPOL],
                jnp.where(lane >= half, pol, raw[:, width - NPOL :]),
            ],
            axis=1,
        )

    @pl.when((layer >= 0) & (layer < radial))
    def _():
        s0[slot, own] = merge(dens[0], polar[0, 0])
        for c in range(3):
            state[1 + c][slot, own] = merge(vel[c, 0], polar[1 + c, 0])
            state[4 + c][slot, own] = mag[c, 0]

    @pl.when((layer < 0) | (layer >= radial))
    def _():
        s0[slot, own] = merge(g2[0, 0], g2p[0, 0])
        s1[slot, own] = merge(g2[0, 1], g2p[0, 1])

    @pl.when((layer == -1) | (layer == radial))
    def _():
        s2[slot, own] = merge(g5[0, 0], g5p[0, 0])
        s3[slot, own] = merge(g5[0, 1], g5p[0, 1])
        for c in range(3):
            state[4 + c][slot, own] = g5[0, 2 + c]

    @pl.when(layer == radial + 1)
    def _():
        s4[slot, own] = gbr[...]

    @pl.when((layer >= -1) & (layer <= radial + 1))
    def _():
        low = merge(side[0, 0, :8], sidep[0, 0])
        high = merge(side[1, 0, :8], sidep[1, 0])
        for f, row, count in PRIM_ROWS:
            state[f][slot, FRONT - count : FRONT] = low[row : row + count]
            state[f][slot, FRONT + azimuth : FRONT + azimuth + count] = high[row : row + count]
        for f, row, count in MAG_ROWS_LOW:
            state[f][slot, FRONT - count : FRONT] = side[0, 0, row : row + count]
        for f, row, count in MAG_ROWS_HIGH:
            state[f][slot, FRONT + azimuth : FRONT + azimuth + count] = side[
                1, 0, row : row + count
            ]

    shape = (TILE, width)
    lane = lax.broadcasted_iota(jnp.int32, shape, 1)
    sub = lax.broadcasted_iota(jnp.int32, shape, 0)

    def shifted(ref, index, base, off):
        here = ref[index, pl.ds(base, TILE), :]
        if off > 0:
            other = ref[index, pl.ds(base + TILE, TILE), :]
            return pltpu.roll(jnp.where(sub < off, other, here), TILE - off, 0)
        if off < 0:
            other = ref[index, pl.ds(base - TILE, TILE), :]
            return pltpu.roll(jnp.where(sub >= TILE + off, other, here), -off, 0)
        return here

    def at(ref, d, base, off=0):
        return shifted(ref, lax.rem(t - 3 + d + 8, 8), base, off)

    def up(x):
        return jnp.where(lane == width - 1, x, pltpu.roll(x, width - 1, 1))

    def down(x):
        return jnp.where(lane == 0, x, pltpu.roll(x, 1, 1))

    def before(x, previous):
        return jnp.where(sub == 0, pltpu.roll(previous, 1, 0), pltpu.roll(x, 1, 0))

    def azimuth_step(base, right_rho, right_u):
        left_r, next_r = edges([at(s0, 0, base, o) for o in (-1, 0, 1, 2, 3)])
        left_u, next_u = edges([at(s3, 0, base, o) for o in (-1, 0, 1, 2, 3)])
        flux = hll_flux(before(next_r, right_rho), left_r, before(next_u, right_u), left_u)
        return next_r, next_u, flux

    def theta_edges(q):
        below = down(q)
        face = interface_value(down(below), below, q, up(q))
        above = jnp.where(lane == width - 1, q, pltpu.roll(face, width - 1, 1))
        return limited(q, face, above)

    here = lax.rem(t, 4)

    def emf_tile(j, _):
        base = pl.multiple_of(FRONT - TILE + j * TILE, TILE)
        u_r, u_t, u_p = (at(s, 1, base) for s in (s1, s2, s3))
        b_r = 0.5 * (at(s4, 1, base) + at(s4, 2, base))
        b_t = at(s5, 1, base)
        b_t = 0.5 * (b_t + up(b_t))
        b_p = 0.5 * (at(s6, 1, base) + at(s6, 1, base, 1))
        rows = pl.ds(base, TILE)
        er[here, rows, :] = u_p * b_t - u_t * b_p
        et[here, rows, :] = u_r * b_p - u_p * b_r
        ep[here, rows, :] = u_t * b_r - u_r * b_t
        return 0

    @pl.when(t >= 4)
    def _():
        lax.fori_loop(0, azimuth // TILE + 2, emf_tile, 0)

    def emf(ref, d, base, off=0):
        return shifted(ref, lax.rem(t - 1 + d + 4, 4), base, off)

    def tile(j, carry):
        right_rho, right_u, flux_low = carry
        start = pl.multiple_of(j * TILE, TILE)
        base = pl.multiple_of(FRONT + j * TILE, TILE)
        rows = pl.ds(start, TILE)

        left_r, right_r = edges([at(s0, d, base) for d in (-1, 0, 1, 2, 3)])
        left_u, right_v = edges([at(s1, d, base) for d in (-1, 0, 1, 2, 3)])
        flux = hll_flux(carry_rho[rows, :], left_r, carry_u[rows, :], left_u)
        total = COURANT_RAD * (flux - carry_flux[rows, :])
        carry_rho[rows, :] = right_r
        carry_u[rows, :] = right_v
        carry_flux[rows, :] = flux

        right_rho, right_u, flux = azimuth_step(base, right_rho, right_u)
        total = total + COURANT_AZI * (flux - before(flux, flux_low))
        flux_low = flux

        rho = at(s0, 0, base)
        left_r, right_r = theta_edges(rho)
        left_u, right_v = theta_edges(at(s2, 0, base))
        theta_flux = hll_flux(down(right_r), left_r, down(right_v), left_u)
        theta_flux = jnp.where(lane == 0, 0.0, theta_flux)
        above = jnp.where(lane == width - 1, 0.0, pltpu.roll(theta_flux, width - 1, 1))
        total = total + COURANT_POL * (above - theta_flux)
        dens_out[0, rows, :] = rho - total

        er_low, er_here, er_high = (emf(er, 0, base, o) for o in (-1, 0, 1))
        ep_low, ep_here, ep_high = (emf(ep, d, base) for d in (-1, 0, 1))
        below_k = emf(et, -1, base, -1)
        edge_a = 0.5 * (ep_low + ep_here)
        edge_r = 0.5 * (er_low + er_here)
        mixed = (0.5 * COURANT_RAD) * (ep_high - ep_low) - (0.5 * COURANT_AZI) * (er_high - er_low)
        across = emf(et, -1, base, 1) + emf(et, 0, base, 1) - below_k - emf(et, 0, base, -1)
        along = emf(et, 1, base, -1) + emf(et, 1, base) - below_k - emf(et, -1, base)
        mag_out[0, 0, rows, :] = (
            at(s4, 0, base)
            - (0.5 * COURANT_POL) * (up(edge_a) - down(edge_a))
            + (0.25 * COURANT_AZI) * across
        )
        mag_out[1, 0, rows, :] = at(s5, 0, base) + 0.5 * (down(mixed) + mixed)
        mag_out[2, 0, rows, :] = (
            at(s6, 0, base)
            - (0.25 * COURANT_RAD) * along
            + (0.5 * COURANT_POL) * (up(edge_r) - down(edge_r))
        )
        return right_rho, right_u, flux_low

    @pl.when(t >= 4)
    def _():
        zero = jnp.zeros(shape, jnp.float32)
        first = azimuth_step(FRONT - TILE, zero, zero)
        lax.fori_loop(0, azimuth // TILE, tile, first)


def stencil(density, velocity, magnetic, polar, ghosts):
    radial, azimuth, width = density.shape
    g2, g2p, g5, g5p, gbr, side, sidep = ghosts

    def own(t):
        return jnp.clip(t - 3, 0, radial - 1)

    def outer(t):
        return jnp.where(t < 3, t, jnp.clip(t - radial, 2, 5))

    def near(t):
        return jnp.where(t < radial + 3, 0, 1)

    def flank(t):
        return jnp.clip(t - 2, 0, radial + 2)

    def out(t):
        return jnp.clip(t - 6, 0, radial - 1)

    rows = FRONT + azimuth + 2 * TILE
    scratch = (
        [pltpu.VMEM((8, rows, width), jnp.float32)] * 7
        + [pltpu.VMEM((4, rows, width), jnp.float32)] * 3
        + [pltpu.VMEM((azimuth, width), jnp.float32)] * 3
    )
    return pl.pallas_call(
        lambda *refs: stencil_kernel(radial, azimuth, *refs),
        grid=(radial + 6,),
        in_specs=[
            pl.BlockSpec((1, azimuth, width), lambda t: (own(t), 0, 0)),
            pl.BlockSpec((3, 1, azimuth, width), lambda t: (0, own(t), 0, 0)),
            pl.BlockSpec((3, 1, azimuth, width), lambda t: (0, own(t), 0, 0)),
            pl.BlockSpec((4, 1, azimuth, NPOL), lambda t: (0, own(t), 0, 0)),
            pl.BlockSpec((1, 2, azimuth, width), lambda t: (outer(t), 0, 0, 0)),
            pl.BlockSpec((1, 2, azimuth, NPOL), lambda t: (outer(t), 0, 0, 0)),
            pl.BlockSpec((1, 5, azimuth, width), lambda t: (near(t), 0, 0, 0)),
            pl.BlockSpec((1, 2, azimuth, NPOL), lambda t: (near(t), 0, 0, 0)),
            pl.BlockSpec((azimuth, width), lambda t: (0, 0)),
            pl.BlockSpec((2, 1, PACKED, width), lambda t: (0, flank(t), 0, 0)),
            pl.BlockSpec((2, 1, 8, NPOL), lambda t: (0, flank(t), 0, 0)),
        ],
        out_specs=[
            pl.BlockSpec((1, azimuth, width), lambda t: (out(t), 0, 0)),
            pl.BlockSpec((3, 1, azimuth, width), lambda t: (0, out(t), 0, 0)),
        ],
        out_shape=[
            jax.ShapeDtypeStruct(density.shape, jnp.float32),
            jax.ShapeDtypeStruct(magnetic.shape, jnp.float32),
        ],
        scratch_shapes=scratch,
        compiler_params=pltpu.CompilerParams(
            dimension_semantics=("arbitrary",), vmem_limit_bytes=62 * 1024 * 1024
        ),
        name="section",
    )(density, velocity, magnetic, polar, g2, g2p, g5, g5p, gbr, side, sidep)


def chain(devices, wrap):
    up = [(i, (i + 1) % devices) for i in range(devices if wrap else devices - 1)]
    return up, [(j, i) for i, j in up]


def radial_ghosts(prim, mag):
    rho, u_r, u_t, u_p = prim
    radial = rho.shape[0]

    def sides(low, high):
        devices = lax.axis_size("row")
        up, down = chain(devices, False)
        return lax.ppermute(high, "row", up), lax.ppermute(low, "row", down)

    low = [rho[:3], u_r[:3], u_t[:1], u_p[:1]]
    high = [rho[-3:], u_r[-3:], u_t[-1:], u_p[-1:]]
    if mag is not None:
        low += [mag[0][:2], mag[1][:1], mag[2][:1]]
        high += [mag[0][-1:], mag[1][-1:], mag[2][-1:]]
    below, above = sides(jnp.concatenate(low, 0), jnp.concatenate(high, 0))
    first = lax.axis_index("row") == 0
    last = lax.axis_index("row") == lax.axis_size("row") - 1

    below = jnp.where(first, jnp.concatenate(repeated(high, prim, mag, 0), 0), below)
    above = jnp.where(last, jnp.concatenate(repeated(low, prim, mag, radial - 1), 0), above)
    outer = jnp.stack(
        [jnp.stack([below[i], below[3 + i]]) for i in range(3)]
        + [jnp.stack([above[i], above[3 + i]]) for i in range(3)]
    )
    if mag is None:
        near = jnp.stack([below[6:8], above[6:8]])
        return outer, near, None
    near = jnp.stack([below[6:11], jnp.concatenate([above[6:9], above[10:12]])])
    return outer, near, above[9]


def repeated(parts, prim, mag, layer):
    fields = list(prim) + ([] if mag is None else list(mag))
    return [jnp.broadcast_to(f[layer], p.shape) for f, p in zip(fields, parts)]


def azimuth_ghosts(prim, mag, outer, near, beyond):
    def rows(sl):
        groups = [
            (prim[0], outer[2, 0], outer[3, 0], 3),
            (prim[3], near[0, 1], near[1, 1], 3),
            (prim[1], outer[2, 1], outer[3, 1], 1),
            (prim[2], near[0, 0], near[1, 0], 1),
        ]
        if mag is not None:
            groups += [(mag[c], near[0, 2 + c], near[1, 2 + c], 1 if c < 2 else 2) for c in range(3)]
        parts = []
        for n, (field, below, above, count) in enumerate(groups):
            pick = sl(count)
            extra = beyond if (beyond is not None and n == 4) else above
            parts.append(
                jnp.concatenate(
                    [below[None, pick], field[:, pick], above[None, pick], extra[None, pick]], 0
                )
            )
        packed = jnp.concatenate(parts, 1)
        size = 8 if mag is None else PACKED
        return jnp.pad(packed, ((0, 0), (0, size - packed.shape[1]), (0, 0)))

    azimuth = prim[0].shape[1]
    up, down = chain(lax.axis_size("phi"), True)
    high = rows(lambda n: slice(azimuth - (1 if n == 2 else n), azimuth))
    low = rows(lambda n: slice(0, n))
    return jnp.stack([lax.ppermute(high, "phi", up), lax.ppermute(low, "phi", down)])


def per_device(density, velocity, magnetic):
    radial, azimuth, width = density.shape
    half = NPOL // 2
    devices = lax.axis_size("phi")
    prim = [density, velocity[0], velocity[1], velocity[2]]
    mag = [magnetic[0], magnetic[1], magnetic[2]]
    rows = jnp.stack(
        [jnp.concatenate([p[..., :half], p[..., width - half :]], axis=-1) for p in prim]
    )
    lines = rows.reshape(devices, -1, azimuth, NPOL)
    lines = lax.all_to_all(lines, "phi", split_axis=0, concat_axis=0, tiled=True)
    lines = filter_lines(lines, width)
    lines = lax.all_to_all(lines, "phi", split_axis=0, concat_axis=0, tiled=True)
    polar = lines.reshape(4, radial, azimuth, NPOL)

    g2, g5, gbr = radial_ghosts(prim, mag)
    side = azimuth_ghosts(prim, mag, g2, g5, gbr)
    smooth = [polar[c] for c in range(4)]
    g2p, g5p, _ = radial_ghosts(smooth, None)
    sidep = azimuth_ghosts(smooth, None, g2p, g5p, None)
    return tuple(
        stencil(density, velocity, magnetic, polar, (g2, g2p, g5, g5p, gbr, side, sidep))
    )


def solution(mesh):
    placed = (P("row", "phi", None), P(None, "row", "phi", None), P(None, "row", "phi", None))
    return jax.shard_map(
        per_device,
        mesh=mesh,
        in_specs=placed,
        out_specs=(P("row", "phi", None), P(None, "row", "phi", None)),
        check_vma=False,
    )
```

```python
import math

import jax
import jax.numpy as jnp
import numpy as np
from jax import lax
from jax.experimental import pallas as pl
from jax.experimental.pallas import tpu as pltpu
from jax.sharding import PartitionSpec as P

NPOL = 128
RADIX = 16
FRONT = 16
TILE = 8

COURANT_RAD = 0.3
COURANT_POL = 0.25
COURANT_AZI = 0.35
SOUND_SPEED = 1.0


def rotate(value, angle):
    re, im = value
    c, s = math.cos(angle), math.sin(angle)
    if im is None:
        return (re * c, re * s)
    return (re * c - im * s, re * s + im * c)


def add(a, b, sign=1.0):
    def part(x, y):
        if y is None:
            return x
        if x is None:
            return y if sign > 0 else -y
        return x + y if sign > 0 else x - y

    return (part(a[0], b[0]), part(a[1], b[1]))


def conj(a):
    return (a[0], None if a[1] is None else -a[1])


def real_fft(xs):
    n = len(xs)
    if n == 1:
        return [(xs[0], None)]
    if n == 2:
        return [(xs[0] + xs[1], None), (xs[0] - xs[1], None)]
    even, odd = real_fft(xs[0::2]), real_fft(xs[1::2])
    half = n // 2

    def at(spec, k):
        return spec[k] if k <= half // 2 else conj(spec[half - k])

    result = []
    for k in range(half + 1):
        e, o = at(even, k % half), at(odd, k % half)
        if k == 0:
            result.append(add(e, o))
        elif k == half:
            result.append(add(e, o, -1.0))
        elif 4 * k == n:
            result.append((e[0], -o[0]))
        else:
            result.append(add(e, rotate(o, -2.0 * math.pi * k / n)))
    return result


def real_ifft(spec, n):
    if n == 2:
        a, b = spec[0][0], spec[1][0]
        return [a + b, a - b]
    half = n // 2
    even, odd = [], []
    for k in range(half // 2 + 1):
        a, b = spec[k], conj(spec[half - k])
        if k == 0:
            a, b = (spec[0][0], None), (spec[half][0], None)
            even.append(add(a, b))
            odd.append(add(a, b, -1.0))
        elif 4 * k == n:
            even.append((2.0 * spec[k][0], None))
            odd.append((-2.0 * spec[k][1], None))
        else:
            even.append(add(a, b))
            odd.append(rotate(add(a, b, -1.0), 2.0 * math.pi * k / n))
    evens, odds = real_ifft(even, half), real_ifft(odd, half)
    return [v for pair in zip(evens, odds) for v in pair]


def filter_tables(cells, theta_count):
    inner = cells // RADIX
    half_polar = NPOL // 2
    k2 = np.arange(RADIX // 2 + 1)[:, None]
    mode = k2 + RADIX * np.arange(inner)[None, :]
    angle = 2.0 * np.pi / cells * ((mode[:, :, None] * np.arange(inner)) % cells)
    cos, sin = np.cos(angle), np.sin(angle)
    forward = np.concatenate(
        [np.concatenate([cos, sin], 2), np.concatenate([-sin, cos], 2)], 1
    ).astype(np.float32)
    rows = np.arange(NPOL)
    theta = np.where(rows < half_polar, rows, theta_count - NPOL + rows)
    row_square = np.sin(np.pi * (theta + 0.5) / theta_count) ** 2
    edge = np.sin(np.pi * (half_polar + 0.5) / theta_count)
    mode_square = (edge * np.sin(np.pi * mode / cells)) ** 2
    damping = row_square / np.maximum(row_square, mode_square[:, :, None])
    return forward, (damping / cells).astype(np.float32)


def filter_kernel(group, inner, blocks, x_ref, basis_ref, damp_ref, out_ref):
    azimuth = x_ref.shape[2]

    def slab(d):
        parts = [
            x_ref[d * blocks : (d + 1) * blocks, g].reshape(inner, NPOL) for g in range(group)
        ]
        return jnp.concatenate(parts, axis=1) if group > 1 else parts[0]

    spectrum = real_fft([slab(d) for d in range(RADIX)])
    filtered = []
    for k, (re, im) in enumerate(spectrum):
        basis = basis_ref[k]
        if im is None:
            forward = basis[:, :inner]
            stacked = re
        else:
            forward = basis
            stacked = jnp.concatenate([re, im], axis=0)
        modes = jnp.dot(
            forward, stacked, precision=lax.Precision.HIGHEST, preferred_element_type=jnp.float32
        )
        damp = damp_ref[k]
        damp = jnp.concatenate([damp, damp], axis=0)
        if group > 1:
            damp = jnp.concatenate([damp] * group, axis=1)
        back = lax.dot_general(
            forward,
            modes * damp,
            (((0,), (0,)), ((), ())),
            precision=lax.Precision.HIGHEST,
            preferred_element_type=jnp.float32,
        )
        filtered.append((back, None) if im is None else (back[:inner], back[inner:]))
    for d, value in enumerate(real_ifft(filtered, RADIX)):
        for g in range(group):
            out_ref[d * blocks : (d + 1) * blocks, g] = value[
                :, g * NPOL : (g + 1) * NPOL
            ].reshape(blocks, azimuth, NPOL)


def filter_lines(lines, theta_count):
    devices, pairs, azimuth, _ = lines.shape
    cells = devices * azimuth
    inner = cells // RADIX
    blocks = inner // azimuth
    group = 2 if pairs % 2 == 0 else 1
    forward, damping = filter_tables(cells, theta_count)
    spec = pl.BlockSpec((devices, group, azimuth, NPOL), lambda p: (0, p, 0, 0))
    return pl.pallas_call(
        lambda *refs: filter_kernel(group, inner, blocks, *refs),
        grid=(pairs // group,),
        in_specs=[
            spec,
            pl.BlockSpec(forward.shape, lambda p: (0, 0, 0)),
            pl.BlockSpec(damping.shape, lambda p: (0, 0, 0)),
        ],
        out_specs=spec,
        out_shape=jax.ShapeDtypeStruct(lines.shape, jnp.float32),
        compiler_params=pltpu.CompilerParams(vmem_limit_bytes=56 * 1024 * 1024),
        name="polar_filter",
    )(lines, jnp.asarray(forward), jnp.asarray(damping))


def interface_value(outer_left, inner_left, inner_right, outer_right):
    guess = 7.0 / 12.0 * (inner_left + inner_right) - 1.0 / 12.0 * (outer_left + outer_right)
    low = jnp.minimum(inner_left, inner_right)
    return jnp.minimum(jnp.maximum(guess, low), jnp.maximum(inner_left, inner_right))


def limited(centre, left_face, right_face):
    to_left = left_face - centre
    to_right = right_face - centre
    reach_right = 2.0 * jnp.abs(to_right)
    reach_left = 2.0 * jnp.abs(to_left)
    left = jnp.minimum(jnp.maximum(to_left, -reach_right), reach_right)
    right = jnp.minimum(jnp.maximum(to_right, -reach_left), reach_left)
    return centre + left, centre + right


def edges(q):
    left_face = interface_value(q[0], q[1], q[2], q[3])
    right_face = interface_value(q[1], q[2], q[3], q[4])
    return limited(q[2], left_face, right_face)


def hll_flux(dens_left, dens_right, speed_left, speed_right):
    slowest = jnp.minimum(jnp.minimum(speed_left, speed_right) - SOUND_SPEED, 0.0)
    fastest = jnp.maximum(jnp.maximum(speed_left, speed_right) + SOUND_SPEED, 0.0)
    upwind = fastest * dens_left * speed_left - slowest * dens_right * speed_right
    return (upwind + slowest * fastest * (dens_right - dens_left)) / (fastest - slowest)


PRIM_ROWS = ((0, 0, 3), (3, 3, 3), (1, 6, 1), (2, 7, 1))
MAG_ROWS_LOW = ((4, 8, 1), (5, 9, 1), (6, 10, 1))
MAG_ROWS_HIGH = ((4, 8, 1), (5, 9, 1), (6, 10, 2))
PACKED = 16


def stencil_kernel(
    radial, azimuth, dens, vel, mag, polar, g2, g2p, g5, g5p, gbr, side, sidep,
    dens_out, mag_out,
    s0, s1, s2, s3, s4, s5, s6, er, et, ep, carry_rho, carry_u, carry_flux,
):
    state = (s0, s1, s2, s3, s4, s5, s6)
    t = pl.program_id(0)
    layer = t - 3
    width = dens.shape[-1]
    half = NPOL // 2
    slot = lax.rem(t, 8)
    own = slice(FRONT, FRONT + azimuth)

    def merge(raw, pol):
        lane = lax.broadcasted_iota(jnp.int32, pol.shape, 1)
        return jnp.concatenate(
            [
                jnp.where(lane < half, pol, raw[:, :NPOL]),
                raw[:, NPOL : width - NPOL],
                jnp.where(lane >= half, pol, raw[:, width - NPOL :]),
            ],
            axis=1,
        )

    @pl.when((layer >= 0) & (layer < radial))
    def _():
        s0[slot, own] = merge(dens[0], polar[0, 0])
        for c in range(3):
            state[1 + c][slot, own] = merge(vel[c, 0], polar[1 + c, 0])
            state[4 + c][slot, own] = mag[c, 0]

    @pl.when((layer < 0) | (layer >= radial))
    def _():
        s0[slot, own] = merge(g2[0, 0], g2p[0, 0])
        s1[slot, own] = merge(g2[0, 1], g2p[0, 1])

    @pl.when((layer == -1) | (layer == radial))
    def _():
        s2[slot, own] = merge(g5[0, 0], g5p[0, 0])
        s3[slot, own] = merge(g5[0, 1], g5p[0, 1])
        for c in range(3):
            state[4 + c][slot, own] = g5[0, 2 + c]

    @pl.when(layer == radial + 1)
    def _():
        s4[slot, own] = gbr[...]

    @pl.when((layer >= -1) & (layer <= radial + 1))
    def _():
        low = merge(side[0, 0, :8], sidep[0, 0])
        high = merge(side[1, 0, :8], sidep[1, 0])
        for f, row, count in PRIM_ROWS:
            state[f][slot, FRONT - count : FRONT] = low[row : row + count]
            state[f][slot, FRONT + azimuth : FRONT + azimuth + count] = high[row : row + count]
        for f, row, count in MAG_ROWS_LOW:
            state[f][slot, FRONT - count : FRONT] = side[0, 0, row : row + count]
        for f, row, count in MAG_ROWS_HIGH:
            state[f][slot, FRONT + azimuth : FRONT + azimuth + count] = side[
                1, 0, row : row + count
            ]

    shape = (TILE, width)
    lane = lax.broadcasted_iota(jnp.int32, shape, 1)
    sub = lax.broadcasted_iota(jnp.int32, shape, 0)

    def shifted(ref, index, base, off):
        here = ref[index, pl.ds(base, TILE), :]
        if off > 0:
            other = ref[index, pl.ds(base + TILE, TILE), :]
            return pltpu.roll(jnp.where(sub < off, other, here), TILE - off, 0)
        if off < 0:
            other = ref[index, pl.ds(base - TILE, TILE), :]
            return pltpu.roll(jnp.where(sub >= TILE + off, other, here), -off, 0)
        return here

    def at(ref, d, base, off=0):
        return shifted(ref, lax.rem(t - 3 + d + 8, 8), base, off)

    def up(x):
        return jnp.where(lane == width - 1, x, pltpu.roll(x, width - 1, 1))

    def down(x):
        return jnp.where(lane == 0, x, pltpu.roll(x, 1, 1))

    def before(x, previous):
        return jnp.where(sub == 0, pltpu.roll(previous, 1, 0), pltpu.roll(x, 1, 0))

    def azimuth_step(base, right_rho, right_u):
        left_r, next_r = edges([at(s0, 0, base, o) for o in (-1, 0, 1, 2, 3)])
        left_u, next_u = edges([at(s3, 0, base, o) for o in (-1, 0, 1, 2, 3)])
        flux = hll_flux(before(next_r, right_rho), left_r, before(next_u, right_u), left_u)
        return next_r, next_u, flux

    def theta_edges(q):
        below = down(q)
        face = interface_value(down(below), below, q, up(q))
        above = jnp.where(lane == width - 1, q, pltpu.roll(face, width - 1, 1))
        return limited(q, face, above)

    here = lax.rem(t, 4)

    def emf_tile(j, _):
        base = pl.multiple_of(FRONT - TILE + j * TILE, TILE)
        u_r, u_t, u_p = (at(s, 1, base) for s in (s1, s2, s3))
        b_r = 0.5 * (at(s4, 1, base) + at(s4, 2, base))
        b_t = at(s5, 1, base)
        b_t = 0.5 * (b_t + up(b_t))
        b_p = 0.5 * (at(s6, 1, base) + at(s6, 1, base, 1))
        rows = pl.ds(base, TILE)
        er[here, rows, :] = u_p * b_t - u_t * b_p
        et[here, rows, :] = u_r * b_p - u_p * b_r
        ep[here, rows, :] = u_t * b_r - u_r * b_t
        return 0

    @pl.when(t >= 4)
    def _():
        lax.fori_loop(0, azimuth // TILE + 2, emf_tile, 0)

    def emf(ref, d, base, off=0):
        return shifted(ref, lax.rem(t - 1 + d + 4, 4), base, off)

    def tile(j, carry):
        right_rho, right_u, flux_low = carry
        start = pl.multiple_of(j * TILE, TILE)
        base = pl.multiple_of(FRONT + j * TILE, TILE)
        rows = pl.ds(start, TILE)

        left_r, right_r = edges([at(s0, d, base) for d in (-1, 0, 1, 2, 3)])
        left_u, right_v = edges([at(s1, d, base) for d in (-1, 0, 1, 2, 3)])
        flux = hll_flux(carry_rho[rows, :], left_r, carry_u[rows, :], left_u)
        total = COURANT_RAD * (flux - carry_flux[rows, :])
        carry_rho[rows, :] = right_r
        carry_u[rows, :] = right_v
        carry_flux[rows, :] = flux

        right_rho, right_u, flux = azimuth_step(base, right_rho, right_u)
        total = total + COURANT_AZI * (flux - before(flux, flux_low))
        flux_low = flux

        rho = at(s0, 0, base)
        left_r, right_r = theta_edges(rho)
        left_u, right_v = theta_edges(at(s2, 0, base))
        theta_flux = hll_flux(down(right_r), left_r, down(right_v), left_u)
        theta_flux = jnp.where(lane == 0, 0.0, theta_flux)
        above = jnp.where(lane == width - 1, 0.0, pltpu.roll(theta_flux, width - 1, 1))
        total = total + COURANT_POL * (above - theta_flux)
        dens_out[0, rows, :] = rho - total

        er_low, er_here, er_high = (emf(er, 0, base, o) for o in (-1, 0, 1))
        ep_low, ep_here, ep_high = (emf(ep, d, base) for d in (-1, 0, 1))
        below_k = emf(et, -1, base, -1)
        edge_a = 0.5 * (ep_low + ep_here)
        edge_r = 0.5 * (er_low + er_here)
        mixed = (0.5 * COURANT_RAD) * (ep_high - ep_low) - (0.5 * COURANT_AZI) * (er_high - er_low)
        across = emf(et, -1, base, 1) + emf(et, 0, base, 1) - below_k - emf(et, 0, base, -1)
        along = emf(et, 1, base, -1) + emf(et, 1, base) - below_k - emf(et, -1, base)
        mag_out[0, 0, rows, :] = (
            at(s4, 0, base)
            - (0.5 * COURANT_POL) * (up(edge_a) - down(edge_a))
            + (0.25 * COURANT_AZI) * across
        )
        mag_out[1, 0, rows, :] = at(s5, 0, base) + 0.5 * (down(mixed) + mixed)
        mag_out[2, 0, rows, :] = (
            at(s6, 0, base)
            - (0.25 * COURANT_RAD) * along
            + (0.5 * COURANT_POL) * (up(edge_r) - down(edge_r))
        )
        return right_rho, right_u, flux_low

    @pl.when(t >= 4)
    def _():
        zero = jnp.zeros(shape, jnp.float32)
        first = azimuth_step(FRONT - TILE, zero, zero)
        lax.fori_loop(0, azimuth // TILE, tile, first)


def stencil(density, velocity, magnetic, polar, ghosts):
    radial, azimuth, width = density.shape
    g2, g2p, g5, g5p, gbr, side, sidep = ghosts

    def own(t):
        return jnp.clip(t - 3, 0, radial - 1)

    def outer(t):
        return jnp.where(t < 3, t, jnp.clip(t - radial, 2, 5))

    def near(t):
        return jnp.where(t < radial + 3, 0, 1)

    def flank(t):
        return jnp.clip(t - 2, 0, radial + 2)

    def out(t):
        return jnp.clip(t - 6, 0, radial - 1)

    rows = FRONT + azimuth + 2 * TILE
    scratch = (
        [pltpu.VMEM((8, rows, width), jnp.float32)] * 7
        + [pltpu.VMEM((4, rows, width), jnp.float32)] * 3
        + [pltpu.VMEM((azimuth, width), jnp.float32)] * 3
    )
    return pl.pallas_call(
        lambda *refs: stencil_kernel(radial, azimuth, *refs),
        grid=(radial + 6,),
        in_specs=[
            pl.BlockSpec((1, azimuth, width), lambda t: (own(t), 0, 0)),
            pl.BlockSpec((3, 1, azimuth, width), lambda t: (0, own(t), 0, 0)),
            pl.BlockSpec((3, 1, azimuth, width), lambda t: (0, own(t), 0, 0)),
            pl.BlockSpec((4, 1, azimuth, NPOL), lambda t: (0, own(t), 0, 0)),
            pl.BlockSpec((1, 2, azimuth, width), lambda t: (outer(t), 0, 0, 0)),
            pl.BlockSpec((1, 2, azimuth, NPOL), lambda t: (outer(t), 0, 0, 0)),
            pl.BlockSpec((1, 5, azimuth, width), lambda t: (near(t), 0, 0, 0)),
            pl.BlockSpec((1, 2, azimuth, NPOL), lambda t: (near(t), 0, 0, 0)),
            pl.BlockSpec((azimuth, width), lambda t: (0, 0)),
            pl.BlockSpec((2, 1, PACKED, width), lambda t: (0, flank(t), 0, 0)),
            pl.BlockSpec((2, 1, 8, NPOL), lambda t: (0, flank(t), 0, 0)),
        ],
        out_specs=[
            pl.BlockSpec((1, azimuth, width), lambda t: (out(t), 0, 0)),
            pl.BlockSpec((3, 1, azimuth, width), lambda t: (0, out(t), 0, 0)),
        ],
        out_shape=[
            jax.ShapeDtypeStruct(density.shape, jnp.float32),
            jax.ShapeDtypeStruct(magnetic.shape, jnp.float32),
        ],
        scratch_shapes=scratch,
        compiler_params=pltpu.CompilerParams(
            dimension_semantics=("arbitrary",), vmem_limit_bytes=62 * 1024 * 1024
        ),
        name="section",
    )(density, velocity, magnetic, polar, g2, g2p, g5, g5p, gbr, side, sidep)


def chain(devices, wrap):
    up = [(i, (i + 1) % devices) for i in range(devices if wrap else devices - 1)]
    return up, [(j, i) for i, j in up]


def radial_ghosts(prim, mag):
    rho, u_r, u_t, u_p = prim
    radial = rho.shape[0]

    def sides(low, high):
        devices = lax.axis_size("row")
        if devices == 2 and low.shape == high.shape:
            sent = jnp.where(lax.axis_index("row") == 0, high, low)
            got = lax.ppermute(sent, "row", [(0, 1), (1, 0)])
            return got, got
        up, down = chain(devices, False)
        return lax.ppermute(high, "row", up), lax.ppermute(low, "row", down)

    low = [rho[:3], u_r[:3], u_t[:1], u_p[:1]]
    high = [rho[-3:], u_r[-3:], u_t[-1:], u_p[-1:]]
    if mag is not None:
        low += [mag[0][:2], mag[1][:1], mag[2][:1]]
        high += [mag[0][-1:], mag[1][-1:], mag[2][-1:]]
    below, above = sides(jnp.concatenate(low, 0), jnp.concatenate(high, 0))
    first = lax.axis_index("row") == 0
    last = lax.axis_index("row") == lax.axis_size("row") - 1

    below = jnp.where(first, jnp.concatenate(repeated(high, prim, mag, 0), 0), below)
    above = jnp.where(last, jnp.concatenate(repeated(low, prim, mag, radial - 1), 0), above)
    outer = jnp.stack(
        [jnp.stack([below[i], below[3 + i]]) for i in range(3)]
        + [jnp.stack([above[i], above[3 + i]]) for i in range(3)]
    )
    if mag is None:
        near = jnp.stack([below[6:8], above[6:8]])
        return outer, near, None
    near = jnp.stack([below[6:11], jnp.concatenate([above[6:9], above[10:12]])])
    return outer, near, above[9]


def repeated(parts, prim, mag, layer):
    fields = list(prim) + ([] if mag is None else list(mag))
    return [jnp.broadcast_to(f[layer], p.shape) for f, p in zip(fields, parts)]


def azimuth_ghosts(prim, mag, outer, near, beyond):
    def rows(sl):
        groups = [
            (prim[0], outer[2, 0], outer[3, 0], 3),
            (prim[3], near[0, 1], near[1, 1], 3),
            (prim[1], outer[2, 1], outer[3, 1], 1),
            (prim[2], near[0, 0], near[1, 0], 1),
        ]
        if mag is not None:
            groups += [(mag[c], near[0, 2 + c], near[1, 2 + c], 1 if c < 2 else 2) for c in range(3)]
        parts = []
        for n, (field, below, above, count) in enumerate(groups):
            pick = sl(count)
            extra = beyond if (beyond is not None and n == 4) else above
            parts.append(
                jnp.concatenate(
                    [below[None, pick], field[:, pick], above[None, pick], extra[None, pick]], 0
                )
            )
        packed = jnp.concatenate(parts, 1)
        size = 8 if mag is None else PACKED
        return jnp.pad(packed, ((0, 0), (0, size - packed.shape[1]), (0, 0)))

    azimuth = prim[0].shape[1]
    up, down = chain(lax.axis_size("phi"), True)
    high = rows(lambda n: slice(azimuth - (1 if n == 2 else n), azimuth))
    low = rows(lambda n: slice(0, n))
    return jnp.stack([lax.ppermute(high, "phi", up), lax.ppermute(low, "phi", down)])


def per_device(density, velocity, magnetic):
    radial, azimuth, width = density.shape
    half = NPOL // 2
    devices = lax.axis_size("phi")
    prim = [density, velocity[0], velocity[1], velocity[2]]
    mag = [magnetic[0], magnetic[1], magnetic[2]]
    rows = jnp.concatenate(
        [
            jnp.concatenate([p[..., :half], p[..., width - half :]], axis=-1)
            for p in (density[None], velocity)
        ],
        axis=0,
    )
    lines = rows.reshape(devices, -1, azimuth, NPOL)
    lines = lax.all_to_all(lines, "phi", split_axis=0, concat_axis=0, tiled=True)
    lines = filter_lines(lines, width)
    lines = lax.all_to_all(lines, "phi", split_axis=0, concat_axis=0, tiled=True)
    polar = lines.reshape(4, radial, azimuth, NPOL)

    g2, g5, gbr = radial_ghosts(prim, mag)
    side = azimuth_ghosts(prim, mag, g2, g5, gbr)
    smooth = [polar[c] for c in range(4)]
    g2p, g5p, _ = radial_ghosts(smooth, None)
    sidep = azimuth_ghosts(smooth, None, g2p, g5p, None)
    return tuple(
        stencil(density, velocity, magnetic, polar, (g2, g2p, g5, g5p, gbr, side, sidep))
    )


def solution(mesh):
    placed = (P("row", "phi", None), P(None, "row", "phi", None), P(None, "row", "phi", None))
    return jax.shard_map(
        per_device,
        mesh=mesh,
        in_specs=placed,
        out_specs=(P("row", "phi", None), P(None, "row", "phi", None)),
        check_vma=False,
    )
```
